32 devices in a mesh: gx: 4 (over z), gy: 4 (over y, x), gz: 2 (over core).
Axes of the slice: x: 2, y: 2, z: 4, core: 2. Of those that a mesh axis runs over, the one named last changes fastest.
Arguments:
- panels: float32 [4, 32768], P(None, ('gy', 'gz')), may hold values from -2 to 3, as said below
- diagonal: float32 [32768], P(('gy', 'gz')), may hold values from 0.5 to 2
- right_side: float32 [32, 32768], P(None, ('gy', 'gz')), may hold values from -6 to 6
- start_guess: float32 [32, 32768], P(None, ('gy', 'gz')), may hold values from -6 to 6
Outputs:
- solution: float32 [32, 32768], P(None, ('gy', 'gz'))
- residual: float32 [32, 32768], P(None, ('gy', 'gz'))
- history: float32 [4, 32], replicated
The draws below stay inside these ranges and needn't reach their ends.
Inputs may be any that keep to these rules, and one draw needn't show every extreme that they name: `panels`: rows 0 to 2 are centroids of a closed surface around the anchor, row 3 positive areas between 0.3 and 3.
All inputs are finite; a program needn't handle non-finite values.
Results may differ from the reference program's by a relative error of at most 0.00035.
Values sent between devices are 32-bit elements; how exact they have to be, the bound alone decides.
A program may use at most 64 MiB of HBM per device.

```python
import math
import jax
import jax.numpy as jnp
from jax import lax

N = 32768
NRHS = 32
ITERS = 4


def draw_panels(key, part):
    key_dir = jax.random.fold_in(key, 11)
    key_rad = jax.random.fold_in(key, 12)
    key_area = jax.random.fold_in(key, 13)
    direction = jax.random.normal(key_dir, (3, N), jnp.float32)
    direction = direction / jnp.sqrt(jnp.sum(direction * direction, 0, keepdims=True) + 1e-06)
    radius = 1.0 + 0.2 * jax.random.uniform(key_rad, (1, N), jnp.float32)
    centers = direction * radius
    panel_area = jnp.exp(jax.random.uniform(key_area, (1, N), jnp.float32, jnp.log(0.3), jnp.log(3.0)))
    return jnp.concatenate([centers, panel_area], 0).astype(jnp.float32)


def level_of(rng, shape, cuts, least, largest):
    factor_of = 1.0
    for dim, parts in cuts:
        steps = jax.random.uniform(jax.random.fold_in(jax.random.fold_in(rng, 6), dim), (parts,), jnp.float32, least / len(cuts), largest / len(cuts))
        factor_of = factor_of * jnp.repeat(jnp.exp(steps), shape[dim] // parts).reshape((-1,) + (1,) * (len(shape) - 1 - dim))
    return factor_of


def scatter_about(key, shape, spread, bound, shards=(), dtype=jnp.bfloat16):
    drawn = spread * jax.random.normal(key, shape, jnp.float32)
    if shards:
        drawn = drawn * level_of(key, shape, shards, -0.22, 0.18)
    return jnp.clip(drawn, -bound, bound).astype(dtype)


def setup_inputs(seed: int = 0) -> dict:
    arg_keys = jax.random.split(jax.random.key(seed), 5)
    panels = draw_panels(jax.random.fold_in(arg_keys[4], 71), 0)
    diagonal = jnp.clip(jnp.exp(math.log(2.0) - 1.3862944 * jax.random.uniform(arg_keys[1], (N,), jnp.float32) ** level_of(arg_keys[1], (N,), ((0, 8),), -0.2, 0.2)), 0.5, 2.0)
    right_side = scatter_about(arg_keys[2], (NRHS, N), 1.0, 6.0, ((1, 8),), jnp.float32)
    start_guess = scatter_about(arg_keys[3], (NRHS, N), 1.0, 6.0, ((1, 8),), jnp.float32)
    return {"panels": panels, "diagonal": diagonal, "right_side": right_side, "start_guess": start_guess}


soft_sq = 0.0025

def kernel(row_pan, col_pan):
    dist_sq = (row_pan[0][:, None] - col_pan[0][None, :]) ** 2
    dist_sq = dist_sq + (row_pan[1][:, None] - col_pan[1][None, :]) ** 2
    dist_sq = dist_sq + (row_pan[2][:, None] - col_pan[2][None, :]) ** 2
    weight = (row_pan[3] * N ** (-0.5))[:, None] * col_pan[3][None, :]
    return weight * lax.rsqrt(dist_sq + soft_sq)

def apply_operator(panels, diagonal, vector):
    row_len = min(N, 1024)
    blocks = panels.reshape(4, N // row_len, row_len).transpose(1, 0, 2)

    def one_block(row_pan):
        return lax.dot_general(vector, kernel(row_pan, panels), (((1,), (1,)), ((), ())), precision=lax.Precision.HIGHEST)
    products = lax.map(one_block, blocks)
    products = products.transpose(1, 0, 2).reshape(vector.shape[0], N)
    return diagonal[None, :] * vector + products

def reference(panels, diagonal, right_side, start_guess):
    residual = right_side - apply_operator(panels, diagonal, start_guess)
    image_res = apply_operator(panels, diagonal, residual)
    solution = start_guess
    direction = jnp.zeros_like(residual)
    sdir = jnp.zeros_like(residual)
    zdir = jnp.zeros_like(residual)
    gamma_prev = jnp.ones((NRHS,), jnp.float32)
    alpha_prev = jnp.ones((NRHS,), jnp.float32)
    records = []
    for turn_index in range(ITERS):
        gamma_now = lax.optimization_barrier(jnp.sum(residual * residual, 1))
        delta_now = lax.optimization_barrier(jnp.sum(image_res * residual, 1))
        omega_now = lax.optimization_barrier(jnp.sum(image_res * image_res, 1))
        fresh = apply_operator(panels, diagonal, image_res)
        records.append(jnp.sqrt(omega_now / gamma_now))
        if turn_index == 0:
            beta_now = jnp.zeros((NRHS,), jnp.float32)
            alpha_now = gamma_now / delta_now
        else:
            beta_now = gamma_now / gamma_prev
            alpha_now = gamma_now / (delta_now - beta_now * gamma_now / alpha_prev)
        beta_col = beta_now[:, None]
        alpha_col = alpha_now[:, None]
        zdir = fresh + beta_col * zdir
        sdir = image_res + beta_col * sdir
        direction = residual + beta_col * direction
        solution = solution + alpha_col * direction
        residual = residual - alpha_col * sdir
        image_res = image_res - alpha_col * zdir
        gamma_prev = gamma_now
        alpha_prev = alpha_now
    return (solution, residual, jnp.stack(records))
```

```python
import functools

import jax
import jax.numpy as jnp
from jax import lax
from jax.experimental import pallas as pl
from jax.experimental.pallas import tpu as pltpu
from jax.sharding import PartitionSpec as P

ITERS = 4
soft_sq = 0.0025
PLANE = ("gy", "gz")
MESH = pl.DeviceIdType.MESH
NEAR = 2


def three(value):
    high = lax.reduce_precision(value, 8, 7)
    rest = value - high
    mid = lax.reduce_precision(rest, 8, 7)
    return high, mid, lax.reduce_precision(rest - mid, 8, 7)


def features(row_pan, col_pan):
    left, right = [], []
    for axis in range(3):
        r = three(row_pan[axis])
        c = three(-2.0 * col_pan[axis])
        for i in range(3):
            for j in range(3):
                if i + j < 4:
                    left.append(r[i])
                    right.append(c[j])
    r_sq = three(jnp.sum(row_pan[:3] ** 2, 0))
    c_sq = three(jnp.sum(col_pan[:3] ** 2, 0) + soft_sq)
    one_r, one_c = jnp.ones_like(row_pan[0]), jnp.ones_like(col_pan[0])
    for i in range(3):
        left += [r_sq[i], one_r]
        right += [one_c, c_sq[i]]
    left += [jnp.zeros_like(one_r)] * 2
    right += [jnp.zeros_like(one_c)] * 2
    return jnp.stack(left).astype(jnp.bfloat16), jnp.stack(right).astype(jnp.bfloat16)


def flip(index, offset, count):
    result = 0
    bit = 1
    while bit < count:
        a = lax.rem(lax.div(index, bit), 2)
        b = (offset // bit) % 2 if isinstance(offset, int) else lax.rem(lax.div(offset, bit), 2)
        result = result + lax.rem(a + b, 2) * bit
        bit *= 2
    return result


def solve_kernel(
    depth, lines, cores, tile,
    b_ref, start_ref, scaled_ref, area_ref, diag_ref, left_ref, right_ref,
    sol_out, res_out, hist_out,
    vec, sol, res, img, direc, sdir, zdir, prev,
    sent, held, parts, near_sum, chunk, chunk_in, sums, sums_in, sums_mid, sums_mid_in,
    vec_send, vec_recv, chunk_send, chunk_recv,
    one_send, one_recv, two_send, two_recv, out_send, out_recv,
):
    plane = lines * cores
    cases, width = b_ref.shape
    step_cols = min(256, width)
    per = width // step_cols
    gx = lax.axis_index("gx")
    gy = lax.axis_index("gy")
    gz = lax.axis_index("gz")
    mine = gy * cores + gz

    def in_plane(k):
        q = flip(mine, k, plane)
        return (gx, lax.div(q, cores), lax.rem(q, cores))

    def in_line(k):
        return (flip(gx, k, depth), gy, gz)

    barrier = pltpu.get_barrier_semaphore()
    for k in range(1, plane):
        pl.semaphore_signal(barrier, inc=1, device_id=in_plane(k), device_id_type=MESH)
    for k in range(1, depth):
        pl.semaphore_signal(barrier, inc=1, device_id=in_line(k), device_id_type=MESH)
    pl.semaphore_wait(barrier, plane - 1 + depth - 1)

    def vec_copy(par, k):
        return pltpu.make_async_remote_copy(
            src_ref=sent.at[par], dst_ref=held.at[par, k - 1],
            send_sem=vec_send.at[par, k - 1], recv_sem=vec_recv.at[par, k - 1],
            device_id=in_plane(k), device_id_type=MESH)

    def chunk_copy(par, k):
        return pltpu.make_async_remote_copy(
            src_ref=chunk.at[par, k], dst_ref=chunk_in.at[par, k],
            send_sem=chunk_send.at[par, k], recv_sem=chunk_recv.at[par, k],
            device_id=in_line(k), device_id_type=MESH)

    def one_copy(par, k):
        return pltpu.make_async_remote_copy(
            src_ref=sums.at[par], dst_ref=sums_in.at[par, gx],
            send_sem=one_send.at[par, k - 1], recv_sem=one_recv.at[par, k - 1],
            device_id=in_line(k), device_id_type=MESH)

    def two_copy(par, k):
        return pltpu.make_async_remote_copy(
            src_ref=sums_mid.at[par], dst_ref=sums_mid_in.at[par, mine],
            send_sem=two_send.at[par, k - 1], recv_sem=two_recv.at[par, k - 1],
            device_id=in_plane(k), device_id_type=MESH)

    def split(k, value):
        high = value.astype(jnp.bfloat16)
        rest = value - high.astype(jnp.float32)
        mid = rest.astype(jnp.bfloat16)
        parts[k, :cases] = high
        parts[k, cases:2 * cases] = mid
        parts[k, 2 * cases:] = (rest - mid.astype(jnp.float32)).astype(jnp.bfloat16)

    def sweep(blocks, col):
        right = right_ref[:, pl.ds(col, step_cols)]
        full = jnp.zeros((3 * cases, step_cols), jnp.float32)
        low_sum = jnp.zeros((cases, step_cols), jnp.float32)
        for k in blocks:
            base = flip(mine, k, plane) * width
            for sub in range(width // tile):
                left = left_ref[pl.ds(pl.multiple_of(base + sub * tile, tile), tile), :]
                value = lax.rsqrt(jnp.dot(left, right, preferred_element_type=jnp.float32))
                high = value.astype(jnp.bfloat16)
                low = (value - high.astype(jnp.float32)).astype(jnp.bfloat16)
                x_all = parts[k, :, sub * tile:(sub + 1) * tile]
                full = full + jnp.dot(x_all, high, preferred_element_type=jnp.float32)
                low_sum = low_sum + jnp.dot(x_all[:cases], low, preferred_element_type=jnp.float32)
        return full[:cases] + (full[cases:2 * cases] + (full[2 * cases:] + low_sum))

    def sums_start_one(par):
        lane = lax.broadcasted_iota(jnp.int32, (cases, 128), 1)
        r, w = res[...], img[...]
        gamma = jnp.sum(r * r, 1, keepdims=True)
        delta = jnp.sum(w * r, 1, keepdims=True)
        omega = jnp.sum(w * w, 1, keepdims=True)
        packed = jnp.where(lane == 0, gamma, jnp.where(lane == 1, delta, omega))
        sums[par] = packed
        sums_in[par, gx] = packed
        for k in range(1, depth):
            one_copy(par, k).start()

    def sums_start_two(par):
        for k in range(1, depth):
            one_copy(par, k).wait()
        total = sums_in[par, 0]
        for g in range(1, depth):
            total = total + sums_in[par, g]
        sums_mid[par] = total
        sums_mid_in[par, mine] = total
        for k in range(1, plane):
            two_copy(par, k).start()

    def sums_finish(par):
        for k in range(1, plane):
            two_copy(par, k).wait()
        total = sums_mid_in[par, 0]
        for q in range(1, plane):
            total = total + sums_mid_in[par, q]
        return total

    def factors(total, turn):
        gamma, delta, omega = total[:, 0:1], total[:, 1:2], total[:, 2:3]
        lane = lax.broadcasted_iota(jnp.int32, (cases, 128), 1)
        hist_out[...] = jnp.where(lane == turn, jnp.sqrt(omega / gamma), hist_out[...])
        first = turn == 0
        beta = jnp.where(first, 0.0, gamma / prev[:, 0:1])
        alpha = gamma / jnp.where(first, delta, delta - beta * gamma / prev[:, 1:2])
        prev[...] = jnp.where(lane == 0, gamma, alpha)
        return alpha, beta

    def advance(alpha, beta):
        sdir[...] = img[...] + beta * sdir[...]
        direc[...] = res[...] + beta * direc[...]
        sol[...] = sol[...] + alpha * direc[...]
        res[...] = res[...] - alpha * sdir[...]

    zero = jnp.zeros((cases, width), jnp.float32)
    sol[...] = start_ref[...]
    vec[...] = start_ref[...]
    res[...] = zero
    img[...] = zero
    direc[...] = zero
    sdir[...] = zero
    zdir[...] = zero
    prev[...] = jnp.ones_like(prev)
    hist_out[...] = jnp.zeros_like(hist_out)

    def step(turn, carry):
        par = lax.rem(turn, 2)
        scaled = vec[...] * scaled_ref[...]
        sent[par] = scaled
        for k in range(1, plane):
            vec_copy(par, k).start()
        sums_start_one(par)
        split(0, scaled)
        for k in range(1, NEAR):
            vec_copy(par, k).wait_recv()
            split(k, held[par, k - 1])

        def near(j, carry):
            col = pl.multiple_of(j * step_cols, step_cols)
            near_sum[:, pl.ds(col, step_cols)] = sweep(range(NEAR), col)
            return carry

        lax.fori_loop(0, depth * per, near, 0)
        for k in range(NEAR, plane):
            vec_copy(par, k).wait_recv()
            split(k, held[par, k - 1])
        sums_start_two(par)

        def far(j, carry):
            k = depth - 1 - lax.div(j, per)
            inner = pl.multiple_of(lax.rem(j, per) * step_cols, step_cols)
            col = pl.multiple_of(flip(gx, k, depth) * width + inner, step_cols)
            got = sweep(range(NEAR, plane), col) + near_sum[:, pl.ds(col, step_cols)]
            chunk[par, k, :, pl.ds(inner, step_cols)] = got

            @pl.when(jnp.logical_and(lax.rem(j, per) == per - 1, k > 0))
            def _():
                chunk_copy(par, k).start()
            return carry

        lax.fori_loop(0, depth * per, far, 0)
        total = sums_finish(par)
        summed = chunk[par, 0]
        for k in range(depth - 1, 0, -1):
            chunk_copy(par, k).wait()
            summed = summed + chunk_in[par, k]
        for k in range(1, plane):
            vec_copy(par, k).wait_send()
        image = diag_ref[...] * vec[...] + area_ref[...] * summed

        @pl.when(turn == 0)
        def _():
            res[...] = b_ref[...] - image
            vec[...] = res[...]

        @pl.when(turn == 1)
        def _():
            img[...] = image
            vec[...] = image

        @pl.when(turn > 1)
        def _():
            alpha, beta = factors(total, turn - 2)
            advance(alpha, beta)
            zdir[...] = image + beta * zdir[...]
            img[...] = img[...] - alpha * zdir[...]
            vec[...] = img[...]

        return carry

    turns = ITERS + 1
    lax.fori_loop(0, turns, step, 0)
    par = turns % 2
    sums_start_one(par)
    sums_start_two(par)
    alpha, beta = factors(sums_finish(par), ITERS - 1)
    advance(alpha, beta)

    spot = pl.ds(pl.multiple_of(gx * width, width), width)

    def out_copy(which, src, dst, k):
        return pltpu.make_async_remote_copy(
            src_ref=src, dst_ref=dst.at[:, spot],
            send_sem=out_send.at[which, k - 1], recv_sem=out_recv.at[which, k - 1],
            device_id=in_line(k), device_id_type=MESH)

    for k in range(1, depth):
        out_copy(0, sol, sol_out, k).start()
        out_copy(1, res, res_out, k).start()
    sol_out[:, spot] = sol[...]
    res_out[:, spot] = res[...]
    for k in range(1, depth):
        out_copy(0, sol, sol_out, k).wait()
        out_copy(1, res, res_out, k).wait()


def solve(b_own, start, scaled, area, diag, left, right, depth, lines, cores):
    cases, width = b_own.shape
    plane = lines * cores
    cols = right.shape[1]
    tile = min(256, width)
    f32 = jnp.float32
    state = pltpu.VMEM((cases, width), f32)
    dma = pltpu.SemaphoreType.DMA
    whole = pl.BlockSpec(memory_space=pltpu.VMEM)
    return pl.pallas_call(
        functools.partial(solve_kernel, depth, lines, cores, tile),
        out_shape=(
            jax.ShapeDtypeStruct((cases, cols), f32),
            jax.ShapeDtypeStruct((cases, cols), f32),
            jax.ShapeDtypeStruct((cases, 128), f32),
        ),
        in_specs=[whole] * 7,
        out_specs=(whole,) * 3,
        scratch_shapes=[state] * 7 + [
            pltpu.VMEM((cases, 128), f32),
            pltpu.VMEM((2, cases, width), f32),
            pltpu.VMEM((2, plane - 1, cases, width), f32),
            pltpu.VMEM((plane, 3 * cases, width), jnp.bfloat16),
            pltpu.VMEM((cases, cols), f32),
            pltpu.VMEM((2, depth, cases, width), f32),
            pltpu.VMEM((2, depth, cases, width), f32),
            pltpu.VMEM((2, cases, 128), f32),
            pltpu.VMEM((2, depth, cases, 128), f32),
            pltpu.VMEM((2, cases, 128), f32),
            pltpu.VMEM((2, plane, cases, 128), f32),
            dma((2, plane - 1)), dma((2, plane - 1)),
            dma((2, depth)), dma((2, depth)),
            dma((2, depth - 1)), dma((2, depth - 1)),
            dma((2, plane - 1)), dma((2, plane - 1)),
            dma((2, depth - 1)), dma((2, depth - 1)),
        ],
        compiler_params=pltpu.CompilerParams(
            collective_id=0, has_side_effects=True, vmem_limit_bytes=48 * 1024 * 1024),
    )(b_own, start, scaled, area, diag, left, right)


def on_device(panels, diagonal, right_side, start_guess):
    col_count = panels.shape[1]
    depth = lax.axis_size("gx")
    lines = lax.axis_size("gy")
    cores = lax.axis_size("gz")
    total = col_count * lines * cores
    width = col_count // depth
    mine = lax.axis_index("gx") * width

    def own(value):
        return lax.dynamic_slice_in_dim(value, mine, width, value.ndim - 1)

    pan_own = own(panels)
    diag_own = own(diagonal)[None, :]
    area_own = pan_own[3][None, :]
    scaled_area = area_own * total ** (-0.5)
    row_pan = lax.all_gather(pan_own, PLANE, axis=0)
    row_pan = jnp.swapaxes(row_pan, 0, 1).reshape(4, -1)
    left, right = features(row_pan, panels)
    solution, residual, records = solve(
        own(right_side), own(start_guess), scaled_area, area_own, diag_own,
        left.T, right, depth, lines, cores)
    return solution, residual, records[:, :ITERS].T


def solution(mesh):
    placed = (P(None, PLANE), P(PLANE), P(None, PLANE), P(None, PLANE))
    return jax.shard_map(
        on_device,
        mesh=mesh,
        in_specs=placed,
        out_specs=(P(None, PLANE), P(None, PLANE), P()),
        check_vma=False,
    )
```

```python
import functools

import jax
import jax.numpy as jnp
from jax import lax
from jax.experimental import pallas as pl
from jax.experimental.pallas import tpu as pltpu
from jax.sharding import PartitionSpec as P

ITERS = 4
soft_sq = 0.0025
PLANE = ("gy", "gz")
MESH = pl.DeviceIdType.MESH
NEAR = 2
UNIT = 512
STEP = 512
CACHE_BYTES = 48 * 1024 * 1024


def three(value):
    high = lax.reduce_precision(value, 8, 7)
    rest = value - high
    mid = lax.reduce_precision(rest, 8, 7)
    return high, mid, lax.reduce_precision(rest - mid, 8, 7)


def features(row_pan, col_pan):
    left, right = [], []
    for axis in range(3):
        r = three(row_pan[axis])
        c = three(-2.0 * col_pan[axis])
        for i in range(3):
            for j in range(3):
                if i + j < 4:
                    left.append(r[i])
                    right.append(c[j])
    r_sq = three(jnp.sum(row_pan[:3] ** 2, 0))
    c_sq = three(jnp.sum(col_pan[:3] ** 2, 0) + soft_sq)
    one_r, one_c = jnp.ones_like(row_pan[0]), jnp.ones_like(col_pan[0])
    for i in range(3):
        left += [r_sq[i], one_r]
        right += [one_c, c_sq[i]]
    left += [jnp.zeros_like(one_r)] * 2
    right += [jnp.zeros_like(one_c)] * 2
    return jnp.stack(left).astype(jnp.bfloat16), jnp.stack(right).astype(jnp.bfloat16)


def flip(index, offset, count):
    result = 0
    bit = 1
    while bit < count:
        a = lax.rem(lax.div(index, bit), 2)
        b = (offset // bit) % 2 if isinstance(offset, int) else lax.rem(lax.div(offset, bit), 2)
        result = result + lax.rem(a + b, 2) * bit
        bit *= 2
    return result


def solve_kernel(
    depth, lines, cores, tile, unit, step_cols, kept,
    b_ref, start_ref, scaled_ref, area_ref, diag_ref, left_ref, right_ref,
    sol, res, hist_out,
    vec, zdir, prev, direc, sdir, wide,
    sent, held, parts, chunk, chunk_in, sums, sums_in, sums_mid, sums_mid_in,
    slot_high, slot_low, kept_high, kept_low,
    vec_send, vec_recv, chunk_send, chunk_recv,
    one_send, one_recv, two_send, two_recv, wide_send, wide_recv, start_sem,
):
    plane = lines * cores
    cases, width = b_ref.shape
    halves = width // unit
    per = width // step_cols
    gx = lax.axis_index("gx")
    gy = lax.axis_index("gy")
    gz = lax.axis_index("gz")
    mine = gy * cores + gz
    spot = pl.ds(pl.multiple_of(gx * width, width), width)

    def in_plane(k):
        q = flip(mine, k, plane)
        return (gx, lax.div(q, cores), lax.rem(q, cores))

    def in_line(k):
        return (flip(gx, k, depth), gy, gz)

    barrier = pltpu.get_barrier_semaphore()
    for k in range(1, plane):
        pl.semaphore_signal(barrier, inc=1, device_id=in_plane(k), device_id_type=MESH)
    for k in range(1, depth):
        pl.semaphore_signal(barrier, inc=1, device_id=in_line(k), device_id_type=MESH)
    pl.semaphore_wait(barrier, plane - 1 + depth - 1)

    def relayed(k):
        return k >= cores and k % cores > 0

    def vec_copy(par, k):
        hand = k % cores
        return pltpu.make_async_remote_copy(
            src_ref=held.at[par, k - hand - 1] if relayed(k) else sent.at[par],
            dst_ref=held.at[par, k - 1],
            send_sem=vec_send.at[par, k - 1], recv_sem=vec_recv.at[par, k - 1],
            device_id=in_plane(hand if relayed(k) else k), device_id_type=MESH)

    def wide_copy(par, k):
        return pltpu.make_async_remote_copy(
            src_ref=vec, dst_ref=wide.at[par, gx],
            send_sem=wide_send.at[par, k - 1], recv_sem=wide_recv.at[par, k - 1],
            device_id=in_line(k), device_id_type=MESH)

    def chunk_copy(par, k):
        return pltpu.make_async_remote_copy(
            src_ref=chunk.at[par, k], dst_ref=chunk_in.at[par, k - 1],
            send_sem=chunk_send.at[par, k], recv_sem=chunk_recv.at[par, k],
            device_id=in_line(k), device_id_type=MESH)

    def one_copy(par, k):
        return pltpu.make_async_remote_copy(
            src_ref=sums.at[par], dst_ref=sums_in.at[par, gx],
            send_sem=one_send.at[par, k - 1], recv_sem=one_recv.at[par, k - 1],
            device_id=in_line(k), device_id_type=MESH)

    def two_copy(par, k):
        return pltpu.make_async_remote_copy(
            src_ref=sums_mid.at[par], dst_ref=sums_mid_in.at[par, mine],
            send_sem=two_send.at[par, k - 1], recv_sem=two_recv.at[par, k - 1],
            device_id=in_plane(k), device_id_type=MESH)

    def split(k, value):
        high = value.astype(jnp.bfloat16)
        rest = value - high.astype(jnp.float32)
        mid = rest.astype(jnp.bfloat16)
        parts[k, :cases] = high
        parts[k, cases:2 * cases] = mid
        parts[k, 2 * cases:] = (rest - mid.astype(jnp.float32)).astype(jnp.bfloat16)

    def build(high_ref, low_ref, k, half, col):
        right = right_ref[:, pl.ds(col, step_cols)]
        base = flip(mine, k, plane) * width + half * unit
        for sub in range(unit // tile):
            left = left_ref[:, pl.ds(pl.multiple_of(base + sub * tile, tile), tile)]
            value = lax.rsqrt(lax.dot_general(
                left, right, (((0,), (0,)), ((), ())), preferred_element_type=jnp.float32))
            high = value.astype(jnp.bfloat16)
            high_ref[sub * tile:(sub + 1) * tile, :] = high
            low_ref[sub * tile:(sub + 1) * tile, :] = (
                value - high.astype(jnp.float32)).astype(jnp.bfloat16)

    def apply(sums, high_ref, low_ref, k, half):
        full, low_sum = sums
        x_all = parts[k, :, half * unit:(half + 1) * unit]
        full = full + jnp.dot(x_all, high_ref[...], preferred_element_type=jnp.float32)
        low_sum = low_sum + jnp.dot(
            x_all[:cases], low_ref[...], preferred_element_type=jnp.float32)
        return full, low_sum

    def empty():
        return (jnp.zeros((3 * cases, step_cols), jnp.float32),
                jnp.zeros((cases, step_cols), jnp.float32))

    def joined(sums):
        full, low_sum = sums
        return full[:cases] + (full[cases:2 * cases] + (full[2 * cases:] + low_sum))

    def build_slot(i, who, col):
        build(slot_high[i % 2], slot_low[i % 2], *who, col)

    def apply_slot(sums, i, who):
        return apply(sums, slot_high[i % 2], slot_low[i % 2], *who)

    def kept_at(c, j, half):
        rows = pl.ds(half * unit, unit)
        return kept_high.at[c, j, rows], kept_low.at[c, j, rows]

    def sums_start_one(par):
        lane = lax.broadcasted_iota(jnp.int32, (cases, 128), 1)
        r, w = res[:, spot], vec[...]
        gamma = jnp.sum(r * r, 1, keepdims=True)
        delta = jnp.sum(w * r, 1, keepdims=True)
        omega = jnp.sum(w * w, 1, keepdims=True)
        packed = jnp.where(lane == 0, gamma, jnp.where(lane == 1, delta, omega))
        sums[par] = packed
        sums_in[par, gx] = packed
        for k in range(1, depth):
            one_copy(par, k).start()

    def sums_start_two(par):
        for k in range(1, depth):
            one_copy(par, k).wait()
        total = sums_in[par, 0]
        for g in range(1, depth):
            total = total + sums_in[par, g]
        sums_mid[par] = total
        sums_mid_in[par, mine] = total
        for k in range(1, plane):
            two_copy(par, k).start()

    def sums_finish(par):
        for k in range(1, plane):
            two_copy(par, k).wait()
        total = sums_mid_in[par, 0]
        for q in range(1, plane):
            total = total + sums_mid_in[par, q]
        return total

    def factors(total, turn):
        gamma, delta, omega = total[:, 0:1], total[:, 1:2], total[:, 2:3]
        lane = lax.broadcasted_iota(jnp.int32, (cases, 128), 1)
        hist_out[...] = jnp.where(lane == turn, jnp.sqrt(omega / gamma), hist_out[...])
        first = turn == 0
        beta = jnp.where(first, 0.0, gamma / prev[:, 0:1])
        alpha = gamma / jnp.where(first, delta, delta - beta * gamma / prev[:, 1:2])
        prev[...] = jnp.where(lane == 0, gamma, alpha)
        return alpha, beta

    def wide_start(par):
        wide[par, gx] = vec[...]
        for k in range(1, depth):
            wide_copy(par, k).start()

    def wide_finish(par):
        for k in range(1, depth):
            wide_copy(par, k).wait()

    def advance(par, alpha, beta):
        for g in range(depth):
            cols = slice(g * width, (g + 1) * width)
            turned = wide[par, g] + beta * sdir[g]
            ahead = res[:, cols] + beta * direc[g]
            sdir[g] = turned
            direc[g] = ahead
            sol[:, cols] = sol[:, cols] + alpha * ahead
            res[:, cols] = res[:, cols] - alpha * turned

    fetch = pltpu.make_async_copy(start_ref, sol, start_sem)
    fetch.start()
    fetch.wait()
    vec[...] = sol[:, spot]
    res[...] = jnp.zeros_like(res)
    direc[...] = jnp.zeros_like(direc)
    sdir[...] = jnp.zeros_like(sdir)
    zdir[...] = jnp.zeros_like(zdir)
    prev[...] = jnp.ones_like(prev)
    hist_out[...] = jnp.zeros_like(hist_out)

    def step(turn, carry):
        par = lax.rem(turn, 2)
        scaled = vec[...] * scaled_ref[...]
        sent[par] = scaled
        for k in range(1, plane):
            if not relayed(k):
                vec_copy(par, k).start()
        sums_start_one(par)
        wide_start(par)
        split(0, scaled)
        for k in range(1, NEAR):
            vec_copy(par, k).wait_recv()
            split(k, held[par, k - 1])

        count = depth * per
        first = [(k, h) for k in range(NEAR) for h in range(halves)]
        fresh = [(k, h) for k in range(NEAR + kept, plane) for h in range(halves)]
        known = [(c, h) for c in range(kept) for h in range(halves)]

        def place(j):
            k = depth - 1 - lax.div(j, per)
            inner = pl.multiple_of(lax.rem(j, per) * step_cols, step_cols)
            col = pl.multiple_of(flip(gx, k, depth) * width + inner, step_cols)
            return k, inner, col

        def next_col(j):
            return place(lax.rem(j + 1, count))[2]

        def rolled(sums, units, j, col, extra):
            done = 0
            for i, who in enumerate(units):
                last = i == len(units) - 1
                build_slot(i + 1, units[0 if last else i + 1], next_col(j) if last else col)
                sums = apply_slot(sums, i, who)
                upto = len(extra) * (i + 1) // len(units)
                for c, h in extra[done:upto]:
                    sums = apply(sums, *kept_at(c, j, h), NEAR + c, h)
                done = upto
            for c, h in extra[done:]:
                sums = apply(sums, *kept_at(c, j, h), NEAR + c, h)
            return sums

        def near(j, carry):
            k, inner, col = place(j)
            chunk[par, k, :, pl.ds(inner, step_cols)] = joined(rolled(empty(), first, j, col, []))
            return carry

        build_slot(0, first[0], place(0)[2])
        split_at = count * 3 // 4
        lax.fori_loop(0, split_at, near, 0)
        for k in range(cores, plane, cores):
            vec_copy(par, k).wait_recv()
            for hand in range(1, cores):
                vec_copy(par, k + hand).start()
        for k in range(cores, plane, cores):
            split(k, held[par, k - 1])
        lax.fori_loop(split_at, count, near, 0)
        for k in range(NEAR, plane):
            if k % cores:
                vec_copy(par, k).wait_recv()
                split(k, held[par, k - 1])
        sums_start_two(par)

        if fresh:
            build_slot(0, fresh[0], place(0)[2])

        def far(j, carry):
            k, inner, col = place(j)

            @pl.when(turn == 0)
            def _():
                for c, h in known:
                    build(*kept_at(c, j, h), NEAR + c, h, col)

            chunk[par, k, :, pl.ds(inner, step_cols)] += joined(
                rolled(empty(), fresh, j, col, known))

            @pl.when(jnp.logical_and(lax.rem(j, per) == per - 1, k > 0))
            def _():
                chunk_copy(par, k).start()
            return carry

        lax.fori_loop(0, count, far, 0)
        total = sums_finish(par)
        summed = chunk[par, 0]
        for k in range(depth - 1, 0, -1):
            chunk_copy(par, k).wait()
            summed = summed + chunk_in[par, k - 1]
        for k in range(1, plane):
            vec_copy(par, k).wait_send()
        wide_finish(par)
        image = diag_ref[...] * vec[...] + area_ref[...] * summed

        @pl.when(turn == 0)
        def _():
            vec[...] = b_ref[...] - image

        @pl.when(turn == 1)
        def _():
            for g in range(depth):
                res[:, g * width:(g + 1) * width] = wide[par, g]
            vec[...] = image

        @pl.when(turn > 1)
        def _():
            alpha, beta = factors(total, turn - 2)
            advance(par, alpha, beta)
            turned = image + beta * zdir[...]
            zdir[...] = turned
            vec[...] = vec[...] - alpha * turned

        return carry

    turns = ITERS + 1
    lax.fori_loop(0, turns, step, 0)
    par = turns % 2
    sums_start_one(par)
    wide_start(par)
    sums_start_two(par)
    alpha, beta = factors(sums_finish(par), ITERS - 1)
    wide_finish(par)
    advance(par, alpha, beta)


def solve(b_own, start, scaled, area, diag, left, right, depth, lines, cores):
    cases, width = b_own.shape
    plane = lines * cores
    cols = right.shape[1]
    tile = min(256, width)
    unit = min(UNIT, width)
    step_cols = min(STEP, width)
    kept = min(plane - NEAR, CACHE_BYTES // (4 * width * cols))
    kept -= (plane - NEAR - kept) * (width // unit) % 2
    f32 = jnp.float32
    square = pltpu.VMEM((unit, step_cols), jnp.bfloat16)
    store = pltpu.VMEM((kept, cols // step_cols, width, step_cols), jnp.bfloat16)
    state = pltpu.VMEM((cases, width), f32)
    dma = pltpu.SemaphoreType.DMA
    whole = pl.BlockSpec(memory_space=pltpu.VMEM)
    return pl.pallas_call(
        functools.partial(solve_kernel, depth, lines, cores, tile, unit, step_cols, kept),
        out_shape=(
            jax.ShapeDtypeStruct((cases, cols), f32),
            jax.ShapeDtypeStruct((cases, cols), f32),
            jax.ShapeDtypeStruct((cases, 128), f32),
        ),
        in_specs=[whole, pl.BlockSpec(memory_space=pl.ANY)] + [whole] * 5,
        out_specs=(whole,) * 3,
        scratch_shapes=[
            state, state, pltpu.VMEM((cases, 128), f32),
            pltpu.VMEM((depth, cases, width), f32), pltpu.VMEM((depth, cases, width), f32),
            pltpu.VMEM((2, depth, cases, width), f32),
            pltpu.VMEM((2, cases, width), f32),
            pltpu.VMEM((2, plane - 1, cases, width), f32),
            pltpu.VMEM((plane, 3 * cases, width), jnp.bfloat16),
            pltpu.VMEM((2, depth, cases, width), f32),
            pltpu.VMEM((2, depth - 1, cases, width), f32),
            pltpu.VMEM((2, cases, 128), f32),
            pltpu.VMEM((2, depth, cases, 128), f32),
            pltpu.VMEM((2, cases, 128), f32),
            pltpu.VMEM((2, plane, cases, 128), f32),
            [square] * 2, [square] * 2, store, store,
            dma((2, plane - 1)), dma((2, plane - 1)),
            dma((2, depth)), dma((2, depth)),
            dma((2, depth - 1)), dma((2, depth - 1)),
            dma((2, plane - 1)), dma((2, plane - 1)),
            dma((2, depth - 1)), dma((2, depth - 1)), dma(()),
        ],
        compiler_params=pltpu.CompilerParams(
            collective_id=0, has_side_effects=True, vmem_limit_bytes=67043328),
    )(b_own, start, scaled, area, diag, left, right)


def on_device(panels, diagonal, right_side, start_guess):
    col_count = panels.shape[1]
    depth = lax.axis_size("gx")
    lines = lax.axis_size("gy")
    cores = lax.axis_size("gz")
    total = col_count * lines * cores
    width = col_count // depth
    mine = lax.axis_index("gx") * width

    def own(value):
        return lax.dynamic_slice_in_dim(value, mine, width, value.ndim - 1)

    pan_own = own(panels)
    diag_own = own(diagonal)[None, :]
    area_own = pan_own[3][None, :]
    scaled_area = area_own * total ** (-0.5)
    row_pan = lax.all_gather(pan_own, PLANE, axis=0)
    row_pan = jnp.swapaxes(row_pan, 0, 1).reshape(4, -1)
    left, right = features(row_pan, panels)
    solution, residual, records = solve(
        own(right_side), start_guess, scaled_area, area_own, diag_own,
        left, right, depth, lines, cores)
    return solution, residual, records[:, :ITERS].T


def solution(mesh):
    placed = (P(None, PLANE), P(PLANE), P(None, PLANE), P(None, PLANE))
    return jax.shard_map(
        on_device,
        mesh=mesh,
        in_specs=placed,
        out_specs=(P(None, PLANE), P(None, PLANE), P()),
        check_vma=False,
    )
```

```python
import functools

import jax
import jax.numpy as jnp
from jax import lax
from jax.experimental import pallas as pl
from jax.experimental.pallas import tpu as pltpu
from jax.sharding import PartitionSpec as P

ITERS = 4
soft_sq = 0.0025
PLANE = ("gy", "gz")
MESH = pl.DeviceIdType.MESH
NEAR = 2
UNIT = 512
STEP = 512
CACHE_BYTES = 48 * 1024 * 1024


def three(value):
    high = value.astype(jnp.bfloat16).astype(jnp.float32)
    rest = value - high
    mid = rest.astype(jnp.bfloat16).astype(jnp.float32)
    return high, mid, rest - mid


def features(pan, is_row):
    rows = []
    for axis in range(3):
        value = pan[axis:axis + 1]
        pieces = three(value if is_row else -2.0 * value)
        for i in range(3):
            for j in range(3):
                if i + j < 4:
                    rows.append(pieces[i if is_row else j])
    square = pan[0:1] * pan[0:1] + pan[1:2] * pan[1:2] + pan[2:3] * pan[2:3]
    one = jnp.ones_like(square)
    for piece in three(square if is_row else square + soft_sq):
        rows += [piece, one] if is_row else [one, piece]
    return rows + [jnp.zeros_like(one)] * 2


def flip(index, offset, count):
    result = 0
    bit = 1
    while bit < count:
        a = lax.rem(lax.div(index, bit), 2)
        b = (offset // bit) % 2 if isinstance(offset, int) else lax.rem(lax.div(offset, bit), 2)
        result = result + lax.rem(a + b, 2) * bit
        bit *= 2
    return result


def solve_kernel(
    depth, lines, cores, tile, unit, step_cols, kept,
    pan_ref, diag_ref, b_any, start_any,
    sol, res, hist_out,
    pan_own, pan_held, feat, left_ref, right_ref, b_ref,
    vec, zdir, prev, direc, sdir, wide,
    sent, held, parts, chunk, chunk_in, sums, sums_in, sums_mid, sums_mid_in,
    slot_high, slot_low, kept_high, kept_low,
    vec_send, vec_recv, chunk_send, chunk_recv,
    one_send, one_recv, two_send, two_recv, wide_send, wide_recv, pan_send, pan_recv, load_sem,
):
    plane = lines * cores
    cases, width = vec.shape
    halves = width // unit
    per = width // step_cols
    gx = lax.axis_index("gx")
    gy = lax.axis_index("gy")
    gz = lax.axis_index("gz")
    mine = gy * cores + gz
    spot = pl.ds(pl.multiple_of(gx * width, width), width)

    def in_plane(k):
        q = flip(mine, k, plane)
        return (gx, lax.div(q, cores), lax.rem(q, cores))

    def in_line(k):
        return (flip(gx, k, depth), gy, gz)

    barrier = pltpu.get_barrier_semaphore()
    for k in range(1, plane):
        pl.semaphore_signal(barrier, inc=1, device_id=in_plane(k), device_id_type=MESH)
    for k in range(1, depth):
        pl.semaphore_signal(barrier, inc=1, device_id=in_line(k), device_id_type=MESH)
    pl.semaphore_wait(barrier, plane - 1 + depth - 1)

    loads = (pltpu.make_async_copy(start_any, sol, load_sem.at[0]),
             pltpu.make_async_copy(b_any.at[:, spot], b_ref, load_sem.at[1]))
    for load in loads:
        load.start()

    def pan_copy(k):
        return pltpu.make_async_remote_copy(
            src_ref=pan_own, dst_ref=pan_held.at[k - 1],
            send_sem=pan_send.at[k - 1], recv_sem=pan_recv.at[k - 1],
            device_id=in_plane(k), device_id_type=MESH)

    def fill(dst, index, pan, is_row):
        for i, row in enumerate(features(pan, is_row)):
            feat[i:i + 1, :] = row
        dst[:, index * width:(index + 1) * width] = feat[...].astype(jnp.bfloat16)

    def fill_from(k):
        pan_copy(k).wait_recv()
        fill(left_ref, k, pan_held[k - 1], True)

    pan_own[...] = pan_ref[:, spot]
    for k in range(1, plane):
        pan_copy(k).start()

    def relayed(k):
        return k >= cores and k % cores > 0

    def vec_copy(par, k):
        hand = k % cores
        return pltpu.make_async_remote_copy(
            src_ref=held.at[par, k - hand - 1] if relayed(k) else sent.at[par],
            dst_ref=held.at[par, k - 1],
            send_sem=vec_send.at[par, k - 1], recv_sem=vec_recv.at[par, k - 1],
            device_id=in_plane(hand if relayed(k) else k), device_id_type=MESH)

    def wide_copy(par, k):
        return pltpu.make_async_remote_copy(
            src_ref=vec, dst_ref=wide.at[par, gx],
            send_sem=wide_send.at[par, k - 1], recv_sem=wide_recv.at[par, k - 1],
            device_id=in_line(k), device_id_type=MESH)

    def chunk_copy(par, k):
        return pltpu.make_async_remote_copy(
            src_ref=chunk.at[par, k], dst_ref=chunk_in.at[par, k - 1],
            send_sem=chunk_send.at[par, k], recv_sem=chunk_recv.at[par, k],
            device_id=in_line(k), device_id_type=MESH)

    def one_copy(par, k):
        return pltpu.make_async_remote_copy(
            src_ref=sums.at[par], dst_ref=sums_in.at[par, gx],
            send_sem=one_send.at[par, k - 1], recv_sem=one_recv.at[par, k - 1],
            device_id=in_line(k), device_id_type=MESH)

    def two_copy(par, k):
        return pltpu.make_async_remote_copy(
            src_ref=sums_mid.at[par], dst_ref=sums_mid_in.at[par, mine],
            send_sem=two_send.at[par, k - 1], recv_sem=two_recv.at[par, k - 1],
            device_id=in_plane(k), device_id_type=MESH)

    def split(k, value):
        high = value.astype(jnp.bfloat16)
        rest = value - high.astype(jnp.float32)
        mid = rest.astype(jnp.bfloat16)
        parts[k, :cases] = high
        parts[k, cases:2 * cases] = mid
        parts[k, 2 * cases:] = (rest - mid.astype(jnp.float32)).astype(jnp.bfloat16)

    def build(high_ref, low_ref, k, half, col):
        right = right_ref[:, pl.ds(col, step_cols)]
        base = k * width + half * unit
        for sub in range(unit // tile):
            left = left_ref[:, base + sub * tile:base + (sub + 1) * tile]
            value = lax.rsqrt(lax.dot_general(
                left, right, (((0,), (0,)), ((), ())), preferred_element_type=jnp.float32))
            high = value.astype(jnp.bfloat16)
            high_ref[sub * tile:(sub + 1) * tile, :] = high
            low_ref[sub * tile:(sub + 1) * tile, :] = (
                value - high.astype(jnp.float32)).astype(jnp.bfloat16)

    def apply(sums, high_ref, low_ref, k, half):
        full, low_sum = sums
        x_all = parts[k, :, half * unit:(half + 1) * unit]
        full = full + jnp.dot(x_all, high_ref[...], preferred_element_type=jnp.float32)
        low_sum = low_sum + jnp.dot(
            x_all[:cases], low_ref[...], preferred_element_type=jnp.float32)
        return full, low_sum

    def empty():
        return (jnp.zeros((3 * cases, step_cols), jnp.float32),
                jnp.zeros((cases, step_cols), jnp.float32))

    def joined(sums):
        full, low_sum = sums
        return full[:cases] + (full[cases:2 * cases] + (full[2 * cases:] + low_sum))

    def build_slot(i, who, col):
        build(slot_high[i % 2], slot_low[i % 2], *who, col)

    def apply_slot(sums, i, who):
        return apply(sums, slot_high[i % 2], slot_low[i % 2], *who)

    def kept_at(c, j, half):
        rows = pl.ds(half * unit, unit)
        return kept_high.at[c, j, rows], kept_low.at[c, j, rows]

    def sums_start_one(par):
        lane = lax.broadcasted_iota(jnp.int32, (cases, 128), 1)
        r, w = res[:, spot], vec[...]
        gamma = jnp.sum(r * r, 1, keepdims=True)
        delta = jnp.sum(w * r, 1, keepdims=True)
        omega = jnp.sum(w * w, 1, keepdims=True)
        packed = jnp.where(lane == 0, gamma, jnp.where(lane == 1, delta, omega))
        sums[par] = packed
        sums_in[par, gx] = packed
        for k in range(1, depth):
            one_copy(par, k).start()

    def sums_start_two(par):
        for k in range(1, depth):
            one_copy(par, k).wait()
        total = sums_in[par, 0]
        for g in range(1, depth):
            total = total + sums_in[par, g]
        sums_mid[par] = total
        sums_mid_in[par, mine] = total
        for k in range(1, plane):
            two_copy(par, k).start()

    def sums_finish(par):
        for k in range(1, plane):
            two_copy(par, k).wait()
        total = sums_mid_in[par, 0]
        for q in range(1, plane):
            total = total + sums_mid_in[par, q]
        return total

    def factors(total, turn):
        gamma, delta, omega = total[:, 0:1], total[:, 1:2], total[:, 2:3]
        lane = lax.broadcasted_iota(jnp.int32, (cases, 128), 1)
        hist_out[...] = jnp.where(lane == turn, jnp.sqrt(omega / gamma), hist_out[...])
        first = turn == 0
        beta = jnp.where(first, 0.0, gamma / prev[:, 0:1])
        alpha = gamma / jnp.where(first, delta, delta - beta * gamma / prev[:, 1:2])
        prev[...] = jnp.where(lane == 0, gamma, alpha)
        return alpha, beta

    def wide_start(par):
        wide[par, gx] = vec[...]
        for k in range(1, depth):
            wide_copy(par, k).start()

    def wide_finish(par):
        for k in range(1, depth):
            wide_copy(par, k).wait()

    def advance(par, alpha, beta):
        for g in range(depth):
            cols = slice(g * width, (g + 1) * width)
            turned = wide[par, g] + beta * sdir[g]
            ahead = res[:, cols] + beta * direc[g]
            sdir[g] = turned
            direc[g] = ahead
            sol[:, cols] = sol[:, cols] + alpha * ahead
            res[:, cols] = res[:, cols] - alpha * turned

    res[...] = jnp.zeros_like(res)
    direc[...] = jnp.zeros_like(direc)
    sdir[...] = jnp.zeros_like(sdir)
    zdir[...] = jnp.zeros_like(zdir)
    prev[...] = jnp.ones_like(prev)
    hist_out[...] = jnp.zeros_like(hist_out)
    for g in range(depth):
        fill(right_ref, g, pan_ref[:, g * width:(g + 1) * width], False)
    fill(left_ref, 0, pan_own[...], True)
    for k in range(1, NEAR):
        fill_from(k)
    for load in loads:
        load.wait()
    vec[...] = sol[:, spot]

    def step(turn, carry):
        par = lax.rem(turn, 2)
        scaled = vec[...] * (pan_own[3:4, :] * (plane * depth * width) ** (-0.5))
        sent[par] = scaled
        for k in range(1, plane):
            if not relayed(k):
                vec_copy(par, k).start()
        sums_start_one(par)
        wide_start(par)
        split(0, scaled)
        for k in range(1, NEAR):
            vec_copy(par, k).wait_recv()
            split(k, held[par, k - 1])

        count = depth * per
        first = [(k, h) for k in range(NEAR) for h in range(halves)]
        fresh = [(k, h) for k in range(NEAR + kept, plane) for h in range(halves)]
        known = [(c, h) for c in range(kept) for h in range(halves)]

        def place(j):
            k = depth - 1 - lax.div(j, per)
            inner = pl.multiple_of(lax.rem(j, per) * step_cols, step_cols)
            col = pl.multiple_of(flip(gx, k, depth) * width + inner, step_cols)
            return k, inner, col

        def next_col(j):
            return place(lax.rem(j + 1, count))[2]

        def rolled(sums, units, j, col, extra):
            done = 0
            for i, who in enumerate(units):
                last = i == len(units) - 1
                build_slot(i + 1, units[0 if last else i + 1], next_col(j) if last else col)
                sums = apply_slot(sums, i, who)
                upto = len(extra) * (i + 1) // len(units)
                for c, h in extra[done:upto]:
                    sums = apply(sums, *kept_at(c, j, h), NEAR + c, h)
                done = upto
            for c, h in extra[done:]:
                sums = apply(sums, *kept_at(c, j, h), NEAR + c, h)
            return sums

        def near(j, carry):
            k, inner, col = place(j)
            chunk[par, k, :, pl.ds(inner, step_cols)] = joined(rolled(empty(), first, j, col, []))
            return carry

        build_slot(0, first[0], place(0)[2])
        split_at = count * 3 // 4
        lax.fori_loop(0, split_at, near, 0)
        for k in range(cores, plane, cores):
            vec_copy(par, k).wait_recv()
            for hand in range(1, cores):
                vec_copy(par, k + hand).start()
        for k in range(cores, plane, cores):
            split(k, held[par, k - 1])
        lax.fori_loop(split_at, count, near, 0)

        @pl.when(turn == 0)
        def _():
            for k in range(NEAR, plane):
                fill_from(k)

        for k in range(NEAR, plane):
            if k % cores:
                vec_copy(par, k).wait_recv()
                split(k, held[par, k - 1])
        sums_start_two(par)

        if fresh:
            build_slot(0, fresh[0], place(0)[2])

        def far(j, carry):
            k, inner, col = place(j)

            @pl.when(turn == 0)
            def _():
                for c, h in known:
                    build(*kept_at(c, j, h), NEAR + c, h, col)

            chunk[par, k, :, pl.ds(inner, step_cols)] += joined(
                rolled(empty(), fresh, j, col, known))

            @pl.when(jnp.logical_and(lax.rem(j, per) == per - 1, k > 0))
            def _():
                chunk_copy(par, k).start()
            return carry

        lax.fori_loop(0, count, far, 0)
        total = sums_finish(par)
        summed = chunk[par, 0]
        for k in range(depth - 1, 0, -1):
            chunk_copy(par, k).wait()
            summed = summed + chunk_in[par, k - 1]
        for k in range(1, plane):
            vec_copy(par, k).wait_send()
        wide_finish(par)
        image = diag_ref[:, spot] * vec[...] + pan_own[3:4, :] * summed

        @pl.when(turn == 0)
        def _():
            vec[...] = b_ref[...] - image

        @pl.when(turn == 1)
        def _():
            for g in range(depth):
                res[:, g * width:(g + 1) * width] = wide[par, g]
            vec[...] = image

        @pl.when(turn > 1)
        def _():
            alpha, beta = factors(total, turn - 2)
            advance(par, alpha, beta)
            turned = image + beta * zdir[...]
            zdir[...] = turned
            vec[...] = vec[...] - alpha * turned

        return carry

    turns = ITERS + 1
    lax.fori_loop(0, turns, step, 0)
    par = turns % 2
    sums_start_one(par)
    wide_start(par)
    sums_start_two(par)
    alpha, beta = factors(sums_finish(par), ITERS - 1)
    wide_finish(par)
    advance(par, alpha, beta)
    for k in range(1, plane):
        pan_copy(k).wait_send()


def solve(panels, diagonal, right_side, start, depth, lines, cores):
    cases, cols = right_side.shape
    width = cols // depth
    plane = lines * cores
    tile = min(256, width)
    unit = min(UNIT, width)
    step_cols = min(STEP, width)
    kept = min(plane - NEAR, CACHE_BYTES // (4 * width * cols))
    kept -= (plane - NEAR - kept) * (width // unit) % 2
    f32 = jnp.float32
    square = pltpu.VMEM((unit, step_cols), jnp.bfloat16)
    store = pltpu.VMEM((kept, cols // step_cols, width, step_cols), jnp.bfloat16)
    state = pltpu.VMEM((cases, width), f32)
    dma = pltpu.SemaphoreType.DMA
    whole = pl.BlockSpec(memory_space=pltpu.VMEM)
    return pl.pallas_call(
        functools.partial(solve_kernel, depth, lines, cores, tile, unit, step_cols, kept),
        out_shape=(
            jax.ShapeDtypeStruct((cases, cols), f32),
            jax.ShapeDtypeStruct((cases, cols), f32),
            jax.ShapeDtypeStruct((cases, 128), f32),
        ),
        in_specs=[whole] * 2 + [pl.BlockSpec(memory_space=pl.ANY)] * 2,
        out_specs=(whole,) * 3,
        scratch_shapes=[
            pltpu.VMEM((4, width), f32), pltpu.VMEM((plane - 1, 4, width), f32),
            pltpu.VMEM((32, width), f32), pltpu.VMEM((32, plane * width), jnp.bfloat16),
            pltpu.VMEM((32, cols), jnp.bfloat16), state,
            state, state, pltpu.VMEM((cases, 128), f32),
            pltpu.VMEM((depth, cases, width), f32), pltpu.VMEM((depth, cases, width), f32),
            pltpu.VMEM((2, depth, cases, width), f32),
            pltpu.VMEM((2, cases, width), f32),
            pltpu.VMEM((2, plane - 1, cases, width), f32),
            pltpu.VMEM((plane, 3 * cases, width), jnp.bfloat16),
            pltpu.VMEM((2, depth, cases, width), f32),
            pltpu.VMEM((2, depth - 1, cases, width), f32),
            pltpu.VMEM((2, cases, 128), f32),
            pltpu.VMEM((2, depth, cases, 128), f32),
            pltpu.VMEM((2, cases, 128), f32),
            pltpu.VMEM((2, plane, cases, 128), f32),
            [square] * 2, [square] * 2, store, store,
            dma((2, plane - 1)), dma((2, plane - 1)),
            dma((2, depth)), dma((2, depth)),
            dma((2, depth - 1)), dma((2, depth - 1)),
            dma((2, plane - 1)), dma((2, plane - 1)),
            dma((2, depth - 1)), dma((2, depth - 1)),
            dma((plane - 1,)), dma((plane - 1,)), dma((2,)),
        ],
        compiler_params=pltpu.CompilerParams(
            collective_id=0, has_side_effects=True, vmem_limit_bytes=67043328),
    )(panels, diagonal, right_side, start)


def on_device(panels, diagonal, right_side, start_guess):
    solution, residual, records = solve(
        panels, diagonal[None, :], right_side, start_guess,
        lax.axis_size("gx"), lax.axis_size("gy"), lax.axis_size("gz"))
    return solution, residual, records[:, :ITERS].T


def solution(mesh):
    placed = (P(None, PLANE), P(PLANE), P(None, PLANE), P(None, PLANE))
    return jax.shard_map(
        on_device,
        mesh=mesh,
        in_specs=placed,
        out_specs=(P(None, PLANE), P(None, PLANE), P()),
        check_vma=False,
    )
```
